32 devices in a mesh: section: 2 (over x), tensor: 2 (over y), expert: 8 (over z, core).
Axes of the slice: x: 2, y: 2, z: 4, core: 2. Of those that a mesh axis runs over, the one named last changes fastest.
Arguments:
- saved_inputs: bfloat16 [2, 2, 512, 2048], P('section', None, 'expert', 'tensor'), may hold values from -64 to 64
- cot_in: bfloat16 [2, 512, 2048], P('section', 'expert', 'tensor'), may hold values from -6 to 6
- loss_grad: bfloat16 [512, 2048], P('expert', 'tensor'), may hold values from -6 to 6
- expert_ids: int32 [2, 2, 512, 2], P('section', None, 'expert'), may hold values from 0 to 3, all different within a row; in each aligned block of 64 rows (0 to 63, 64 to 127, ..., all dimensions but the last counted through in order) at most 48 rows name the same one
- route_weights: float32 [2, 2, 512, 2], P('section', None, 'expert'), may hold values from 0.05 to 0.5
- norm_gain: float32 [2, 2048], P('section', 'tensor'), may hold values from 0.12 to 8
- w_gate: bfloat16 [2, 8, 2048, 384], P('section', 'expert', 'tensor'), may hold values from -0.125 to 0.125
- w_up: bfloat16 [2, 8, 2048, 384], P('section', 'expert', 'tensor'), may hold values from -0.125 to 0.125
- w_down: bfloat16 [2, 8, 384, 2048], P('section', 'expert', None, 'tensor'), may hold values from -0.21875 to 0.21875
Outputs:
- input_grads: bfloat16 [2, 2, 512, 2048], P('section', None, 'expert', 'tensor')
The draws below stay inside these ranges and needn't reach their ends.
Inputs may be any that keep to these rules, and one draw needn't show every extreme that they name: `expert_ids`: each row names 2 different experts. Within each aligned block of 64 rows (the rows of one device in one micro-batch of one layer) no expert is named by more than 48 rows, and in some blocks one expert is named by exactly 48.
All inputs are finite; a program needn't handle non-finite values.
Results may differ from the reference program's by a relative error of at most 0.028.
Values may be sent and summed in bfloat16 or wider, within the bound.
A program may use at most 64 MiB of HBM per device.

```python
import math
import jax
import jax.numpy as jnp
import numpy as np
from jax import lax

D = 2048
FF = 768
TOK_MB = 64
LAYERS = 2
EXPERTS = 4
TOP = 2
CAP = 48
TOKENS = 512
N_TENSOR = 2
N_EXPERT = 8


def draw_saved_inputs(key, part):
    key_base, key_cols, key_rows = jax.random.split(key, 3)
    ramp = 3.0 ** (jnp.arange(D, dtype=jnp.float32) / D)
    columns = ramp * 10.0 ** (0.5 * jax.random.uniform(key_cols, (D,), jnp.float32))
    row_scale = 10.0 ** (jax.random.uniform(key_rows, (LAYERS, 2, TOKENS, 1), jnp.float32) - 0.5)
    base = jnp.clip(jax.random.normal(key_base, (LAYERS, 2, TOKENS, D), jnp.float32), -6.0, 6.0)
    return (base * columns * row_scale / 3.0).astype(jnp.bfloat16)


def draw_norm_gain(key, part):
    key_rough = jax.random.fold_in(key, 17)
    place = jnp.arange(D, dtype=jnp.float32) / D
    ramp = 0.25 * 16.0 ** place
    rough = 10.0 ** (0.3 * jax.random.uniform(key_rough, (LAYERS, D), jnp.float32) - 0.15)
    return (ramp[None, :] * rough).astype(jnp.float32)


def block_scale(stream_key, dims, cuts, smallest, top_value):
    def one(dim, blocks):
        steps = jax.random.uniform(jax.random.fold_in(jax.random.fold_in(stream_key, 6), dim), (blocks,), jnp.float32, smallest / len(cuts), top_value / len(cuts))
        return jnp.repeat(jnp.exp(steps), dims[dim] // blocks).reshape((-1,) + (1,) * (len(dims) - dim - 1))

    loudness = one(*cuts[0])
    for cut in cuts[1:]:
        loudness = loudness * one(*cut)
    return loudness


def routed_block(key, own, number, rows, count, top, reach, lean):
    sequence = jax.random.permutation(key, count)
    packed, usual = shares(count, rows * top, reach, lean, True), shares(count, rows * top, reach, lean, False)
    places = jnp.arange(count)

    def named(tallies, rotation):
        used = int((tallies > 0).sum())
        fixed = max(1, used // 4)
        shifted = fixed + (places - fixed + rotation * (used - fixed)) % max(1, count - fixed)
        return jnp.zeros((count,), jnp.int32).at[sequence[jnp.where(places < fixed, places, shifted)]].set(jnp.asarray(tallies, jnp.int32))

    tallies = jnp.where(number % 4 == 0, named(packed, number // 4), named(usual, number - number // 4 - 1))
    mixed = jax.random.permutation(jax.random.fold_in(own, 3), count)
    donor, taker = mixed[0:count // 2 * 2:2], mixed[1:count // 2 * 2:2]
    slack = jnp.minimum(tallies[donor] - 1, reach - tallies[taker]) // 2
    slack = jnp.where((donor == sequence[0]) | (taker == sequence[0]) | (tallies[taker] == 0), 0, jnp.maximum(slack, 0))
    shifted = jax.random.randint(jax.random.fold_in(own, 4), (count // 2,), 0, 1 << 20) % (slack + 1)
    tallies = tallies.at[donor].add(-shifted).at[taker].add(shifted)
    members = jnp.searchsorted(jnp.cumsum(tallies), jnp.arange(rows * top), side="right").astype(jnp.int32)
    listing = members.reshape(top, rows).T
    listing = listing[jax.random.permutation(jax.random.fold_in(own, 1), rows)]
    rotation = jax.random.randint(jax.random.fold_in(own, 2), (rows, 1), 0, top)
    return jnp.take_along_axis(listing, (jnp.arange(top)[None, :] + rotation) % top, axis=1)


def shares(amount, total, bound, lean, full):
    loads = [(1 << 20) // math.isqrt(grade ** lean) + 1 for grade in range(1, amount + 1)]
    largest = bound if full else min(bound, max(-(-total // amount), total * loads[0] // sum(loads)))
    least = 1 if total - largest >= amount - 1 else 0
    holding, rest = [largest] + [least] * (amount - 1), total - largest - least * (amount - 1)
    while rest > 0:
        movable = [i for i in range(1, amount) if holding[i] < largest] or [i for i in range(1, amount) if holding[i] < bound]
        whole, remaining = sum([loads[i] for i in movable]), rest
        for i in movable:
            more = min(bound - holding[i], max(1, remaining * loads[i] // whole), rest)
            holding[i] = holding[i] + more
            rest = rest - more
    return np.array(holding)


def bell_draw(stream_key, shape, width, bound, cuts=(), kind=jnp.bfloat16):
    drawn = jax.random.normal(stream_key, shape, jnp.float32) * width
    if len(cuts) > 0:
        drawn = block_scale(stream_key, shape, cuts, -0.22, 0.18) * drawn
    return jnp.clip(drawn, min=-bound, max=bound).astype(kind)


def setup_inputs(seed: int = 0) -> dict:
    key_of = jax.random.split(jax.random.key(seed), 10)
    saved_inputs = draw_saved_inputs(jax.random.fold_in(key_of[9], 71), 0)
    cot_in = bell_draw(key_of[1], (LAYERS, TOKENS, D), 1.0, 6.0, ((0, 2), (1, 8), (2, 2)))
    loss_grad = bell_draw(key_of[2], (TOKENS, D), 1.0, 6.0, ((0, 8), (1, 2)))
    expert_ids_keys = jax.random.split(jax.random.fold_in(key_of[3], 1), LAYERS * 2 * TOKENS // TOK_MB)
    expert_ids_turns = jax.random.permutation(jax.random.fold_in(key_of[3], 3), LAYERS * 2 * TOKENS // TOK_MB)
    expert_ids = jax.vmap(lambda own, number: routed_block(jax.random.fold_in(key_of[3], 2), own, number, TOK_MB, EXPERTS, TOP, CAP, 2))(expert_ids_keys, expert_ids_turns).reshape((LAYERS, 2, TOKENS, TOP))
    route_weights = jnp.clip(jnp.exp(math.log(0.5) - 2.3025851 * jax.random.uniform(key_of[4], (LAYERS, 2, TOKENS, TOP), jnp.float32) ** block_scale(key_of[4], (LAYERS, 2, TOKENS, TOP), ((0, 2), (2, 8)), -0.2, 0.2)), 0.05, 0.5)
    norm_gain = draw_norm_gain(jax.random.fold_in(key_of[9], 71), 0)
    w_gate = bell_draw(key_of[6], (LAYERS, 2 * EXPERTS, D, FF // 2), D ** -0.5, 0.125, ((0, 2), (1, 8), (2, 2)))
    w_up = bell_draw(key_of[7], (LAYERS, 2 * EXPERTS, D, FF // 2), D ** -0.5, 0.125, ((0, 2), (1, 8), (2, 2)))
    w_down = bell_draw(key_of[8], (LAYERS, 2 * EXPERTS, FF // 2, D), FF ** -0.5, 0.21875, ((0, 2), (1, 8), (3, 2)))
    return {"saved_inputs": saved_inputs, "cot_in": cot_in, "loss_grad": loss_grad, "expert_ids": expert_ids, "route_weights": route_weights, "norm_gain": norm_gain, "w_gate": w_gate, "w_up": w_up, "w_down": w_down}


epsilon = 1e-06

def silu_grad(values):
    sigma = jax.nn.sigmoid(values)
    return sigma * (1.0 + values * (1.0 - sigma))

def product(left, right):
    return jnp.dot(left.astype(jnp.float32), right.astype(jnp.float32), precision=lax.Precision.HIGHEST)

def rounded(values):
    return lax.optimization_barrier(values.astype(jnp.bfloat16)).astype(jnp.float32)

def slot_tables(route_ids, weights):
    blocks = route_ids.reshape(N_EXPERT, TOK_MB * TOP)
    onehot = (blocks[:, :, None] == jnp.arange(EXPERTS, dtype=jnp.int32)[None, None, :]).astype(jnp.int32)
    before = jnp.cumsum(onehot, axis=1) - onehot
    position = lax.optimization_barrier(jnp.sum(before * onehot, axis=2))
    source = jnp.arange(N_EXPERT, dtype=jnp.int32)[:, None]
    flat_slot = (blocks * (N_EXPERT * CAP) + source * CAP + position).reshape(-1).astype(jnp.int32)
    token_index = jnp.repeat(jnp.arange(TOKENS, dtype=jnp.int32), TOP)
    slot_total = EXPERTS * N_EXPERT * CAP
    token_of = jnp.full((slot_total,), TOKENS, jnp.int32).at[flat_slot].set(token_index)
    weight_of = jnp.zeros((slot_total,), jnp.float32).at[flat_slot].set(weights.reshape(-1))
    return (token_of, weight_of)

def expert_back(operands):
    rows_in, rows_grad, gate_weights, up_weights, down_weights = operands
    group = D // N_TENSOR
    pieces = []
    for part_index in range(2):
        gate_sum = jnp.zeros((rows_in.shape[0], FF // 2), jnp.float32)
        up_sum = jnp.zeros((rows_in.shape[0], FF // 2), jnp.float32)
        hidden = jnp.zeros((rows_in.shape[0], FF // 2), jnp.float32)
        for rank_index in range(N_TENSOR):
            low = rank_index * group
            high = low + group
            gate_sum = gate_sum + rounded(product(rows_in[:, low:high], gate_weights[part_index, low:high]))
            up_sum = up_sum + rounded(product(rows_in[:, low:high], up_weights[part_index, low:high]))
            hidden = hidden + rounded(product(rows_grad[:, low:high], down_weights[part_index][:, low:high].T))
        grad_gate = (hidden * up_sum * silu_grad(gate_sum)).astype(jnp.bfloat16)
        grad_up = (hidden * jax.nn.silu(gate_sum)).astype(jnp.bfloat16)
        grad_piece = product(grad_gate, gate_weights[part_index].T) + product(grad_up, up_weights[part_index].T)
        pieces.append(grad_piece.astype(jnp.bfloat16))
    return jnp.stack(pieces)

def layer_back(inputs, incoming, route_ids, weights, gain_row, gate_weights, up_weights, down_weights):
    values = inputs.astype(jnp.float32)
    squares = lax.optimization_barrier(jnp.sum(values * values, axis=1, keepdims=True))
    root_mean = jnp.sqrt(squares / D + epsilon)
    normed = values / root_mean
    expert_input = (normed * gain_row[None, :]).astype(jnp.bfloat16)
    token_of, weight_of = slot_tables(route_ids, weights)
    padded_input = jnp.concatenate([expert_input, jnp.zeros((1, D), jnp.bfloat16)], axis=0)
    padded_grad = jnp.concatenate([incoming, jnp.zeros((1, D), jnp.bfloat16)], axis=0)
    rows_in = padded_input[token_of].reshape(EXPERTS, N_EXPERT * CAP, D)
    rows_grad = (weight_of[:, None] * padded_grad[token_of].astype(jnp.float32)).astype(jnp.bfloat16)
    rows_grad = rows_grad.reshape(EXPERTS, N_EXPERT * CAP, D)
    pieces = lax.map(expert_back, (rows_in, rows_grad, gate_weights.reshape(EXPERTS, 2, D, FF // 2), up_weights.reshape(EXPERTS, 2, D, FF // 2), down_weights.reshape(EXPERTS, 2, FF // 2, D)))
    summed = lax.optimization_barrier(jnp.sum(pieces.astype(jnp.float32), axis=1)).reshape(-1, D)
    cot_normed = jax.ops.segment_sum(summed, token_of, TOKENS + 1)[:TOKENS]
    scaled = gain_row[None, :] * cot_normed
    inner = lax.optimization_barrier(jnp.sum(normed * scaled, axis=1, keepdims=True))
    return (incoming.astype(jnp.float32) + (scaled - normed * (inner / D)) / root_mean).astype(jnp.bfloat16)

def reference(saved_inputs, cot_in, loss_grad, expert_ids, route_weights, norm_gain, w_gate, w_up, w_down):

    def first_layer(layer):
        return layer_back(saved_inputs[layer, 0], cot_in[layer], expert_ids[layer, 0], route_weights[layer, 0], norm_gain[layer], w_gate[layer], w_up[layer], w_down[layer])
    first_pass = lax.map(first_layer, jnp.arange(LAYERS, dtype=jnp.int32))
    following = jnp.concatenate([first_pass[1:], loss_grad[None]], axis=0)

    def second_layer(layer):
        return layer_back(saved_inputs[layer, 1], following[layer], expert_ids[layer, 1], route_weights[layer, 1], norm_gain[layer], w_gate[layer], w_up[layer], w_down[layer])
    second_pass = lax.map(second_layer, jnp.arange(LAYERS, dtype=jnp.int32))
    return jnp.stack([first_pass, second_pass], axis=1)
```

```python
import jax
import jax.numpy as jnp
from jax import lax
from jax.experimental import pallas as pl
from jax.experimental.pallas import tpu as pltpu
from jax.sharding import PartitionSpec as P

epsilon = 1e-06
MESH = pl.DeviceIdType.MESH
bf16 = jnp.bfloat16
f32 = jnp.float32


def contract_last(left, right):
    return lax.dot_general(left, right, (((1,), (1,)), ((), ())), preferred_element_type=f32)


def contract_first(left, right):
    return lax.dot_general(left, right, (((0,), (0,)), ((), ())), preferred_element_type=f32)


def dot(left, right):
    return jnp.dot(left, right, preferred_element_type=f32)


def make_kernel(sections, tensors, experts, capacity):

    def kernel(
        saved, cot_in, loss_grad, ids, weights, gain, wg_hbm, wu_hbm, wd_hbm, out,
        wg, wu, wd, w_sem, choose, picked, rows_out, rows, part_gu, part_h,
        y_send_gu, y_recv_gu, y_send_h, y_recv_h, grads, piece, pair_send, pair_recv,
        ret_send, ret_recv, sq_send, sq_recv, in_send, in_recv, sec_recv,
        d_s, d_r, f_s, f_r, y_s, y_r, a_s, a_r, p_s, p_r, r_s, r_r, q_s, q_r, i_s, i_r, c_s, c_r,
    ):
        s = lax.axis_index("section")
        t = lax.axis_index("tensor")
        x = lax.axis_index("expert")
        e, q = x // 2, x % 2
        ot, oq = 1 - t, 1 - q
        tok = saved.shape[2]
        feat = saved.shape[3]
        top = ids.shape[3]
        hid = wg.shape[1]
        model = feat * tensors

        loads = [
            pltpu.make_async_copy(wd_hbm.at[0, 0], wd, w_sem.at[0]),
            pltpu.make_async_copy(wg_hbm.at[0, 0], wg, w_sem.at[1]),
            pltpu.make_async_copy(wu_hbm.at[0, 0], wu, w_sem.at[2]),
        ]
        for load in loads:
            load.start()

        def expert_at(j):
            return lax.rem(e + j, experts)

        def source_at(j):
            return lax.rem(e + experts - j, experts)

        lane_peer = lambda chip: (s, t, 2 * chip + q)
        partner = (s, t, 2 * e + oq)
        y_peer = (s, ot, x)

        barrier = pltpu.get_barrier_semaphore()
        greet = [lane_peer(expert_at(j)) for j in range(1, experts)] + [partner, y_peer]
        for device in greet:
            pl.semaphore_signal(barrier, inc=1, device_id=device, device_id_type=MESH)

        @pl.when(s > 0)
        def _():
            pl.semaphore_signal(barrier, inc=1, device_id=(s - 1, t, x), device_id_type=MESH)

        @pl.when(s < sections - 1)
        def _():
            pl.semaphore_signal(barrier, inc=1, device_id=(s + 1, t, x), device_id_type=MESH)

        def remote(src, dst, send, recv, device):
            return pltpu.make_async_remote_copy(
                src_ref=src, dst_ref=dst, send_sem=send, recv_sem=recv,
                device_id=device, device_id_type=MESH,
            )

        def direct(m, k, j):
            return remote(
                rows_out.at[m, k, j], rows.at[m, k, j, q], d_s.at[m, k, j], d_r.at[m, k, j],
                lane_peer(expert_at(j)),
            )

        def forward(m, k, j):
            return remote(
                rows.at[m, k, j, q], rows.at[m, k, j, q], f_s.at[m, k, j], f_r.at[m, k, j], partner
            )

        def exchange(m, k, j):
            src, dst = ((y_send_gu, y_recv_gu), (y_send_h, y_recv_h))[k]
            return remote(src.at[m, j], dst.at[m, j], y_s.at[m, k, j], y_r.at[m, k, j], y_peer)

        def share(m, j):
            return remote(
                grads.at[m, j, t], grads.at[m, j, t], a_s.at[m, j], a_r.at[m, j], y_peer
            )

        def pair(m, j):
            return remote(
                pair_send.at[m, j], pair_recv.at[m, j], p_s.at[m, j], p_r.at[m, j], partner
            )

        def give_back(m, j):
            return remote(
                ret_send.at[m, j], ret_recv.at[m, j], r_s.at[m, j], r_r.at[m, j],
                lane_peer(source_at(j)),
            )

        def squares_copy():
            return remote(sq_send, sq_recv, q_s, q_r, y_peer)

        def inner_copy(m):
            return remote(in_send.at[m], in_recv.at[m], i_s.at[m], i_r.at[m], y_peer)

        def section_copy():
            return remote(out.at[0, 0], sec_recv, c_s, c_r, (s - 1, t, x))

        started = []

        def start(copy):
            copy.start()
            started.append(copy)

        lane = lax.broadcasted_iota(jnp.int32, (tok, 128), 1)
        named = e + lane
        named = jnp.where(named >= experts, named - experts, named)
        named = jnp.where(lane < experts, named, -1)
        earlier = (
            lax.broadcasted_iota(jnp.int32, (tok, tok), 1)
            < lax.broadcasted_iota(jnp.int32, (tok, tok), 0)
        ).astype(f32).astype(bf16)
        slot = lax.broadcasted_iota(jnp.int32, (tok, capacity), 1).astype(f32)
        weight_of = []
        for m in range(2):
            hit = jnp.zeros((tok, 128), f32)
            weight = jnp.zeros((tok, 128), f32)
            for k in range(top):
                same = (ids[0, m, :, k : k + 1] == named).astype(f32)
                hit = hit + same
                weight = weight + same * weights[0, m, :, k : k + 1]
            position = dot(earlier, hit.astype(bf16))
            for j in range(experts):
                chosen = (position[:, j : j + 1] == slot).astype(f32) * hit[:, j : j + 1]
                choose[m, j] = chosen.astype(bf16)
            picked[m] = weight
        square = []
        for m in range(2):
            values = saved[0, m].astype(f32)
            square.append(jnp.sum(values * values, axis=1, keepdims=True))
        sq_send[...] = jnp.where(lane < 64, square[0], square[1])

        neighbours = (s > 0).astype(jnp.int32) + (s < sections - 1).astype(jnp.int32)
        pl.semaphore_wait(barrier, len(greet) + neighbours)

        start(squares_copy())

        def dispatch(m, k, value_of):
            for j in list(range(1, experts)) + [0]:
                packed = contract_first(choose[m, j], value_of(j)).astype(bf16)
                if j == 0:
                    rows[m, k, j, q] = packed
                    start(forward(m, k, j))
                else:
                    rows_out[m, k, j] = packed
                    start(direct(m, k, j))

        def dispatch_grads(m, incoming):
            dispatch(m, 1, lambda j: (picked[m][:, j : j + 1] * incoming).astype(bf16))

        dispatch_grads(0, cot_in[0].astype(f32))
        squares_copy().wait_recv()
        total = sq_send[...] + sq_recv[...]
        roots = [
            jnp.sqrt(total[:, 64 * m : 64 * m + 1] / model + epsilon) for m in range(2)
        ]

        def normed_of(m):
            return saved[0, m].astype(f32) / roots[m]

        for m in range(2):
            value = (normed_of(m) * gain[...]).astype(bf16)
            dispatch(m, 0, lambda j: value)

        for load in loads:
            load.wait()

        def receive(m, k, j):
            if j > 0:
                direct(m, k, j).wait_recv()
                start(forward(m, k, j))

        def consume(m, k, j):
            forward(m, k, j).wait_recv()
            flat = rows[m, k, j].reshape(2 * capacity, feat)
            if k == 0:
                part_gu[m, j, :, :, :hid] = dot(flat, wg[...]).reshape(2, capacity, hid)
                part_gu[m, j, :, :, hid:] = dot(flat, wu[...]).reshape(2, capacity, hid)
                y_send_gu[m, j] = part_gu[m, j, ot].astype(bf16)
            else:
                part_h[m, j] = contract_last(flat, wd[...]).reshape(2, capacity, hid)
                y_send_h[m, j] = part_h[m, j, ot].astype(bf16)
            start(exchange(m, k, j))

        def stream(items):
            last = None
            for item in items:
                receive(*item)
                if last is not None:
                    consume(*last)
                last = item
            consume(*last)

        def activate(m, j):
            exchange(m, 0, j).wait_recv()
            exchange(m, 1, j).wait_recv()
            both = part_gu[m, j, t] + y_recv_gu[m, j].astype(f32)
            hidden = part_h[m, j, t] + y_recv_h[m, j].astype(f32)
            gate, up = both[:, :hid], both[:, hid:]
            sigma = jax.nn.sigmoid(gate)
            grads[m, j, t, :, :hid] = (
                hidden * up * (sigma * (1.0 + gate * (1.0 - sigma)))
            ).astype(bf16)
            grads[m, j, t, :, hid:] = (hidden * (gate * sigma)).astype(bf16)
            start(share(m, j))

        def pieces(m, j):
            share(m, j).wait_recv()
            flat = grads[m, j].reshape(2 * capacity, 2 * hid)
            done = contract_last(flat[:, :hid], wg[...]) + contract_last(flat[:, hid:], wu[...])
            piece[m, j] = done.reshape(2, capacity, feat)
            pair_send[m, j] = piece[m, j, oq].astype(bf16)
            start(pair(m, j))

        def finish(m, j):
            pair(m, j).wait_recv()
            summed = (piece[m, j, q] + pair_recv[m, j].astype(f32)).astype(bf16)
            if j == 0:
                ret_recv[m, j] = summed
            else:
                ret_send[m, j] = summed
                start(give_back(m, j))

        def send_back(m):
            order = list(range(1, experts)) + [0]
            last = None
            for j in order:
                pieces(m, j)
                if last is not None:
                    finish(m, last)
                last = j
            finish(m, last)

        def combine(m, incoming):
            cot = dot(choose[m, 0], ret_recv[m, 0])
            for j in range(1, experts):
                give_back(m, j).wait_recv()
                cot = cot + dot(choose[m, j], ret_recv[m, j])
            scaled = gain[...] * cot
            normed = normed_of(m)
            own = jnp.sum(normed * scaled, axis=1, keepdims=True)
            in_send[m] = jnp.broadcast_to(own, (tok, 128))
            start(inner_copy(m))
            inner_copy(m).wait_recv()
            inner = (in_send[m] + in_recv[m])[:, :1]
            out[0, m] = (
                incoming + (scaled - normed * (inner / model)) / roots[m]
            ).astype(bf16)

        js = list(range(experts))
        stream([(0, 1, j) for j in js] + [(0, 0, j) for j in js])
        for j in js[1:] + [0]:
            activate(0, j)
        stream([(1, 0, j) for j in js])
        send_back(0)
        combine(0, cot_in[0].astype(f32))

        @pl.when(s > 0)
        def _():
            section_copy().start()

        @pl.when(s < sections - 1)
        def _():
            section_copy().wait_recv()

        @pl.when(s == sections - 1)
        def _():
            sec_recv[...] = loss_grad[...]

        incoming = sec_recv[...].astype(f32)
        dispatch_grads(1, incoming)
        stream([(1, 1, j) for j in js])
        for j in js[1:] + [0]:
            activate(1, j)
        send_back(1)
        combine(1, incoming)

        for copy in started:
            copy.wait_send()

        @pl.when(s > 0)
        def _():
            section_copy().wait_send()

    return kernel


def solution(mesh):
    sections, tensors = mesh.shape["section"], mesh.shape["tensor"]
    experts = mesh.shape["expert"] // 2

    def local(saved, cot_in, loss_grad, ids, weights, gain, wg, wu, wd):
        tok, feat = saved.shape[2], saved.shape[3]
        hid = wg.shape[3]
        named = 3 * tok * ids.shape[3] // (2 * experts)
        cap = -(-named // 16) * 16
        vmem = pl.BlockSpec(memory_space=pltpu.VMEM)
        hbm = pl.BlockSpec(memory_space=pl.ANY)
        dma = pltpu.SemaphoreType.DMA
        scratch = [
            pltpu.VMEM((feat, hid), bf16), pltpu.VMEM((feat, hid), bf16),
            pltpu.VMEM((hid, feat), bf16), dma((3,)),
            pltpu.VMEM((2, experts, tok, cap), bf16), pltpu.VMEM((2, tok, 128), f32),
            pltpu.VMEM((2, 2, experts, cap, feat), bf16),
            pltpu.VMEM((2, 2, experts, 2, cap, feat), bf16),
            pltpu.VMEM((2, experts, 2, cap, 2 * hid), f32),
            pltpu.VMEM((2, experts, 2, cap, hid), f32),
            pltpu.VMEM((2, experts, cap, 2 * hid), bf16),
            pltpu.VMEM((2, experts, cap, 2 * hid), bf16),
            pltpu.VMEM((2, experts, cap, hid), bf16),
            pltpu.VMEM((2, experts, cap, hid), bf16),
            pltpu.VMEM((2, experts, 2, cap, 2 * hid), bf16),
            pltpu.VMEM((2, experts, 2, cap, feat), f32),
            pltpu.VMEM((2, experts, cap, feat), bf16),
            pltpu.VMEM((2, experts, cap, feat), bf16),
            pltpu.VMEM((2, experts, cap, feat), bf16),
            pltpu.VMEM((2, experts, cap, feat), bf16),
            pltpu.VMEM((tok, 128), f32), pltpu.VMEM((tok, 128), f32),
            pltpu.VMEM((2, tok, 128), f32), pltpu.VMEM((2, tok, 128), f32),
            pltpu.VMEM((tok, feat), bf16),
        ]
        for shape in [(2, 2, experts)] * 6 + [(2, experts)] * 6:
            scratch.append(dma(shape))
        scratch += [dma, dma, dma((2,)), dma((2,)), dma, dma]
        return pl.pallas_call(
            make_kernel(sections, tensors, experts, cap),
            out_shape=jax.ShapeDtypeStruct((1, 2, tok, feat), bf16),
            in_specs=[vmem] * 6 + [hbm] * 3,
            out_specs=vmem,
            scratch_shapes=scratch,
            compiler_params=pltpu.CompilerParams(
                collective_id=0, has_side_effects=True, vmem_limit_bytes=62 * 1024 * 1024
            ),
            name="expert_back",
        )(saved, cot_in, loss_grad, ids, weights, gain, wg, wu, wd)

    in_specs = (
        P("section", None, "expert", "tensor"),
        P("section", "expert", "tensor"),
        P("expert", "tensor"),
        P("section", None, "expert", None),
        P("section", None, "expert", None),
        P("section", "tensor"),
        P("section", "expert", "tensor", None),
        P("section", "expert", "tensor", None),
        P("section", "expert", None, "tensor"),
    )
    out_specs = P("section", None, "expert", "tensor")
    return jax.shard_map(local, mesh=mesh, in_specs=in_specs, out_specs=out_specs, check_vma=False)
```

```python
import jax
import jax.numpy as jnp
from jax import lax
from jax.experimental import pallas as pl
from jax.experimental.pallas import tpu as pltpu
from jax.sharding import PartitionSpec as P

epsilon = 1e-06
MESH = pl.DeviceIdType.MESH
bf16 = jnp.bfloat16
f32 = jnp.float32


def contract_last(left, right):
    return lax.dot_general(left, right, (((1,), (1,)), ((), ())), preferred_element_type=f32)


def contract_first(left, right):
    return lax.dot_general(left, right, (((0,), (0,)), ((), ())), preferred_element_type=f32)


def dot(left, right):
    return jnp.dot(left, right, preferred_element_type=f32)


def make_kernel(sections, tensors, experts, capacity):

    def kernel(
        saved, cot_in, loss_grad, ids, weights, gain, wg_hbm, wu_hbm, wd_hbm, out,
        wg, wu, wd, w_sem, choose, picked, rows_out, rows, part_gu, part_h,
        y_send_gu, y_recv_gu, y_send_h, y_recv_h, grads, piece, pair_send, pair_recv,
        ret_send, ret_recv, sq_send, sq_recv, in_send, in_recv, sec_recv,
        d_s, d_r, f_s, f_r, y_s, y_r, a_s, a_r, p_s, p_r, r_s, r_r, q_s, q_r, i_s, i_r, c_s, c_r,
    ):
        s = lax.axis_index("section")
        t = lax.axis_index("tensor")
        x = lax.axis_index("expert")
        e, q = x // 2, x % 2
        ot, oq = 1 - t, 1 - q
        tok = saved.shape[2]
        feat = saved.shape[3]
        top = ids.shape[2]
        hid = wg.shape[1]
        model = feat * tensors

        loads = [
            pltpu.make_async_copy(wd_hbm.at[0, 0], wd, w_sem.at[0]),
            pltpu.make_async_copy(wg_hbm.at[0, 0], wg, w_sem.at[1]),
            pltpu.make_async_copy(wu_hbm.at[0, 0], wu, w_sem.at[2]),
        ]
        for load in loads:
            load.start()

        def expert_at(j):
            return lax.rem(e + j, experts)

        def source_at(j):
            return lax.rem(e + experts - j, experts)

        lane_peer = lambda chip: (s, t, 2 * chip + q)
        partner = (s, t, 2 * e + oq)
        y_peer = (s, ot, x)

        barrier = pltpu.get_barrier_semaphore()
        greet = [lane_peer(expert_at(j)) for j in range(1, experts)] + [partner, y_peer]
        for device in greet:
            pl.semaphore_signal(barrier, inc=1, device_id=device, device_id_type=MESH)

        @pl.when(s > 0)
        def _():
            pl.semaphore_signal(barrier, inc=1, device_id=(s - 1, t, x), device_id_type=MESH)

        @pl.when(s < sections - 1)
        def _():
            pl.semaphore_signal(barrier, inc=1, device_id=(s + 1, t, x), device_id_type=MESH)

        def remote(src, dst, send, recv, device):
            return pltpu.make_async_remote_copy(
                src_ref=src, dst_ref=dst, send_sem=send, recv_sem=recv,
                device_id=device, device_id_type=MESH,
            )

        def direct(m, k, j):
            return remote(
                rows_out.at[m, k, j], rows.at[m, k, j, q], d_s.at[m, k, j], d_r.at[m, k, j],
                lane_peer(expert_at(j)),
            )

        def forward(m, k, j):
            return remote(
                rows.at[m, k, j, q], rows.at[m, k, j, q], f_s.at[m, k, j], f_r.at[m, k, j], partner
            )

        def exchange(m, k, j):
            src, dst = ((y_send_gu, y_recv_gu), (y_send_h, y_recv_h))[k]
            return remote(src.at[m, j], dst.at[m, j], y_s.at[m, k, j], y_r.at[m, k, j], y_peer)

        def share(m, j):
            return remote(
                grads.at[m, j, t], grads.at[m, j, t], a_s.at[m, j], a_r.at[m, j], y_peer
            )

        def pair(m, j):
            return remote(
                pair_send.at[m, j], pair_recv.at[m, j], p_s.at[m, j], p_r.at[m, j], partner
            )

        def give_back(m, j):
            return remote(
                ret_send.at[m, j], ret_recv.at[m, j], r_s.at[m, j], r_r.at[m, j],
                lane_peer(source_at(j)),
            )

        def squares_copy():
            return remote(sq_send, sq_recv, q_s, q_r, y_peer)

        def inner_copy(m):
            return remote(in_send.at[m], in_recv.at[m], i_s.at[m], i_r.at[m], y_peer)

        def section_copy():
            return remote(out.at[0, 0], sec_recv, c_s, c_r, (s - 1, t, x))

        started = []

        def start(copy):
            copy.start()
            started.append(copy)

        height = max(8, experts)
        lane = lax.broadcasted_iota(jnp.int32, (tok, 128), 1)
        named = e + lax.broadcasted_iota(jnp.int32, (height, tok), 0)
        named = jnp.where(named >= experts, named - experts, named)
        later = (
            lax.broadcasted_iota(jnp.int32, (tok, tok), 0)
            < lax.broadcasted_iota(jnp.int32, (tok, tok), 1)
        ).astype(f32).astype(bf16)
        slot = lax.broadcasted_iota(jnp.int32, (capacity, tok), 0).astype(f32)
        for m in range(2):
            hit = jnp.zeros((height, tok), f32)
            weight = jnp.zeros((height, tok), f32)
            for k in range(top):
                same = (ids[0, m, k : k + 1, :] == named).astype(f32)
                hit = hit + same
                weight = weight + same * weights[0, m, k : k + 1, :]
            position = dot(hit.astype(bf16), later)
            for j in range(experts):
                chosen = (position[j : j + 1] == slot).astype(f32) * hit[j : j + 1]
                choose[m, j] = chosen.astype(bf16)
                picked[m, j] = jnp.broadcast_to(
                    jnp.sum(chosen * weight[j : j + 1], axis=1, keepdims=True), (capacity, 128)
                )
        square = []
        for m in range(2):
            values = saved[0, m].astype(f32)
            square.append(jnp.sum(values * values, axis=1, keepdims=True))
        sq_send[...] = jnp.where(lane < 64, square[0], square[1])

        neighbours = (s > 0).astype(jnp.int32) + (s < sections - 1).astype(jnp.int32)
        pl.semaphore_wait(barrier, len(greet) + neighbours)

        start(squares_copy())

        def dispatch(m, k, j, value):
            packed = dot(choose[m, j], value)
            if k == 1:
                packed = picked[m, j][:, :1] * packed
            if j == 0:
                rows[m, k, j, q] = packed.astype(bf16)
                start(forward(m, k, j))
            else:
                rows_out[m, k, j] = packed.astype(bf16)
                start(direct(m, k, j))

        js = list(range(experts))
        near = js[1 : experts // 2 + 1] + [0]
        far = js[experts // 2 + 1 :]
        for j in near:
            dispatch(0, 1, j, cot_in[0])
        squares_copy().wait_recv()
        total = sq_send[...] + sq_recv[...]
        roots = [
            jnp.sqrt(total[:, 64 * m : 64 * m + 1] / model + epsilon) for m in range(2)
        ]

        def normed_of(m):
            return saved[0, m].astype(f32) / roots[m]

        def expert_input(m):
            return (normed_of(m) * gain[...]).astype(bf16)

        value = expert_input(0)
        for j in near:
            dispatch(0, 0, j, value)
        for j in far:
            dispatch(0, 1, j, cot_in[0])
            dispatch(0, 0, j, value)

        for load in loads:
            load.wait()

        def receive(m, k, j):
            if j > 0:
                direct(m, k, j).wait_recv()
                start(forward(m, k, j))

        def consume(m, k, j):
            forward(m, k, j).wait_recv()
            flat = rows[m, k, j].reshape(2 * capacity, feat)
            if k == 0:
                part_gu[m, j, :, :, :hid] = dot(flat, wg[...]).reshape(2, capacity, hid)
                part_gu[m, j, :, :, hid:] = dot(flat, wu[...]).reshape(2, capacity, hid)
                y_send_gu[m, j] = part_gu[m, j, ot].astype(bf16)
            else:
                part_h[m, j] = contract_last(flat, wd[...]).reshape(2, capacity, hid)
                y_send_h[m, j] = part_h[m, j, ot].astype(bf16)
            start(exchange(m, k, j))

        def stream(items):
            last = None
            for item in items:
                receive(*item)
                if last is not None:
                    consume(*last)
                last = item
            consume(*last)

        def activate(m, j):
            exchange(m, 0, j).wait_recv()
            exchange(m, 1, j).wait_recv()
            both = part_gu[m, j, t] + y_recv_gu[m, j].astype(f32)
            hidden = part_h[m, j, t] + y_recv_h[m, j].astype(f32)
            gate, up = both[:, :hid], both[:, hid:]
            sigma = jax.nn.sigmoid(gate)
            grads[m, j, t, :, :hid] = (
                hidden * up * (sigma * (1.0 + gate * (1.0 - sigma)))
            ).astype(bf16)
            grads[m, j, t, :, hid:] = (hidden * (gate * sigma)).astype(bf16)
            start(share(m, j))

        def pieces(m, j):
            share(m, j).wait_recv()
            flat = grads[m, j].reshape(2 * capacity, 2 * hid)
            done = contract_last(flat[:, :hid], wg[...]) + contract_last(flat[:, hid:], wu[...])
            piece[m, j] = done.reshape(2, capacity, feat)
            pair_send[m, j] = piece[m, j, oq].astype(bf16)
            start(pair(m, j))

        def finish(m, j):
            pair(m, j).wait_recv()
            summed = (piece[m, j, q] + pair_recv[m, j].astype(f32)).astype(bf16)
            if j == 0:
                ret_recv[m, j] = summed
            else:
                ret_send[m, j] = summed
                start(give_back(m, j))

        def pipeline(m, kinds, between=()):
            stream([(m, k, j) for k in kinds for j in js])
            for j in js[1:] + [0]:
                activate(m, j)
            if between:
                stream(between)
            last = None
            for j in js[1:] + [0]:
                pieces(m, j)
                if last is not None:
                    finish(m, last)
                last = j
            finish(m, last)

        def combine(m, incoming):
            cot = contract_first(choose[m, 0], ret_recv[m, 0])
            for j in range(1, experts):
                give_back(m, j).wait_recv()
                cot = cot + contract_first(choose[m, j], ret_recv[m, j])
            scaled = gain[...] * cot
            normed = normed_of(m)
            own = jnp.sum(normed * scaled, axis=1, keepdims=True)
            in_send[m] = jnp.broadcast_to(own, (tok, 128))
            start(inner_copy(m))
            inner_copy(m).wait_recv()
            inner = (in_send[m] + in_recv[m])[:, :1]
            out[0, m] = (
                incoming + (scaled - normed * (inner / model)) / roots[m]
            ).astype(bf16)

        pipeline(0, (1, 0))
        value = expert_input(1)
        for j in js[1:] + [0]:
            dispatch(1, 0, j, value)
        combine(0, cot_in[0].astype(f32))

        @pl.when(s > 0)
        def _():
            section_copy().start()

        stream([(1, 0, j) for j in js[: experts // 2]])

        @pl.when(s < sections - 1)
        def _():
            section_copy().wait_recv()

        @pl.when(s == sections - 1)
        def _():
            sec_recv[...] = loss_grad[...]

        for j in js[1:] + [0]:
            dispatch(1, 1, j, sec_recv[...])
        stream([(1, 0, j) for j in js[experts // 2 :]])
        pipeline(1, (1,))
        combine(1, sec_recv[...].astype(f32))

        for copy in started:
            copy.wait_send()

        @pl.when(s > 0)
        def _():
            section_copy().wait_send()

    return kernel


def solution(mesh):
    sections, tensors = mesh.shape["section"], mesh.shape["tensor"]
    experts = mesh.shape["expert"] // 2

    def local(saved, cot_in, loss_grad, ids, weights, gain, wg, wu, wd):
        tok, feat = saved.shape[2], saved.shape[3]
        hid = wg.shape[3]
        named = 3 * tok * ids.shape[3] // (2 * experts)
        cap = -(-named // 16) * 16
        vmem = pl.BlockSpec(memory_space=pltpu.VMEM)
        hbm = pl.BlockSpec(memory_space=pl.ANY)
        dma = pltpu.SemaphoreType.DMA
        scratch = [
            pltpu.VMEM((feat, hid), bf16), pltpu.VMEM((feat, hid), bf16),
            pltpu.VMEM((hid, feat), bf16), dma((3,)),
            pltpu.VMEM((2, experts, cap, tok), bf16), pltpu.VMEM((2, experts, cap, 128), f32),
            pltpu.VMEM((2, 2, experts, cap, feat), bf16),
            pltpu.VMEM((2, 2, experts, 2, cap, feat), bf16),
            pltpu.VMEM((2, experts, 2, cap, 2 * hid), f32),
            pltpu.VMEM((2, experts, 2, cap, hid), f32),
            pltpu.VMEM((2, experts, cap, 2 * hid), bf16),
            pltpu.VMEM((2, experts, cap, 2 * hid), bf16),
            pltpu.VMEM((2, experts, cap, hid), bf16),
            pltpu.VMEM((2, experts, cap, hid), bf16),
            pltpu.VMEM((2, experts, 2, cap, 2 * hid), bf16),
            pltpu.VMEM((2, experts, 2, cap, feat), f32),
            pltpu.VMEM((2, experts, cap, feat), bf16),
            pltpu.VMEM((2, experts, cap, feat), bf16),
            pltpu.VMEM((2, experts, cap, feat), bf16),
            pltpu.VMEM((2, experts, cap, feat), bf16),
            pltpu.VMEM((tok, 128), f32), pltpu.VMEM((tok, 128), f32),
            pltpu.VMEM((2, tok, 128), f32), pltpu.VMEM((2, tok, 128), f32),
            pltpu.VMEM((tok, feat), bf16),
        ]
        for shape in [(2, 2, experts)] * 6 + [(2, experts)] * 6:
            scratch.append(dma(shape))
        scratch += [dma, dma, dma((2,)), dma((2,)), dma, dma]
        return pl.pallas_call(
            make_kernel(sections, tensors, experts, cap),
            out_shape=jax.ShapeDtypeStruct((1, 2, tok, feat), bf16),
            in_specs=[vmem] * 6 + [hbm] * 3,
            out_specs=vmem,
            scratch_shapes=scratch,
            compiler_params=pltpu.CompilerParams(
                collective_id=0, has_side_effects=True, vmem_limit_bytes=62 * 1024 * 1024
            ),
            name="expert_back",
        )(
            saved, cot_in, loss_grad, ids.transpose(0, 1, 3, 2), weights.transpose(0, 1, 3, 2),
            gain, wg, wu, wd,
        )

    in_specs = (
        P("section", None, "expert", "tensor"),
        P("section", "expert", "tensor"),
        P("expert", "tensor"),
        P("section", None, "expert", None),
        P("section", None, "expert", None),
        P("section", "tensor"),
        P("section", "expert", "tensor", None),
        P("section", "expert", "tensor", None),
        P("section", "expert", None, "tensor"),
    )
    out_specs = P("section", None, "expert", "tensor")
    return jax.shard_map(local, mesh=mesh, in_specs=in_specs, out_specs=out_specs, check_vma=False)
```
